8 devices in a mesh: pod: 1 (over z), data: 2 (over y), expert: 4 (over x, core).
Axes of the slice: x: 2, y: 2, z: 1, core: 2. Of those that a mesh axis runs over, the one named last changes fastest.
Arguments:
- x_tokens: bfloat16 [8192, 1024], P(('pod', 'data', 'expert'))
- sel_tokens: int32 [32, 256], P(('pod', 'expert'), 'data')
- gate_w: float32 [32, 256], P(('pod', 'expert'), 'data')
- w_in: bfloat16 [32, 1024, 4096], P('expert')
- w_out: bfloat16 [32, 4096, 1024], P('expert')
Outputs:
- output: bfloat16 [8192, 1024], P(('pod', 'data', 'expert'))
All inputs are finite; a program needn't handle non-finite values.
Results may differ from the reference program's by a relative error of at most 0.001.
Values are sent between devices in bfloat16 or wider.
A program may use at most 1 GiB of HBM per device.

```python
import jax
import jax.numpy as jnp
from jax import lax

TOK_DEV = 1024
D_MODEL = 1024
FF_DIM = 4096
EXPERTS = 32
CAP_FACTOR = 1
DATA_WAYS = 2
EXPERT_WAYS = 4

SOURCES = DATA_WAYS * EXPERT_WAYS
TOKENS = SOURCES * TOK_DEV
SLOTS = CAP_FACTOR * TOK_DEV
AVG_ROWS = SLOTS // SOURCES
E_LOCAL = EXPERTS // EXPERT_WAYS
C_LOCAL = SLOTS // E_LOCAL
CAPACITY = DATA_WAYS * C_LOCAL


def draw_routes(key):
    key_perm, key_delta, key_shuffle, key_row = jax.random.split(key, 4)
    perms = jax.vmap(lambda sub_key: jax.random.permutation(sub_key, SOURCES))(jax.random.split(key_perm, SOURCES))
    delta = jax.random.randint(key_delta, (SOURCES, SOURCES // 2), -AVG_ROWS, AVG_ROWS + 1)
    delta = delta.at[:, 0].set(AVG_ROWS)
    counts = jnp.concatenate([AVG_ROWS + delta, AVG_ROWS - delta], axis=1)
    bounds = jnp.cumsum(counts, axis=1)
    slot_ids = jnp.arange(SLOTS)
    position = jax.vmap(lambda bound_row: jnp.searchsorted(bound_row, slot_ids, side="right"))(bounds)
    src_dev = jnp.take_along_axis(perms, position, axis=1)
    shuffled = jax.vmap(lambda sub_key, src_row: jax.random.permutation(sub_key, src_row))(jax.random.split(key_shuffle, SOURCES), src_dev)
    row_ids = jax.random.randint(key_row, (SOURCES, SLOTS), 0, TOK_DEV)
    tok_index = shuffled * TOK_DEV + row_ids
    tok_index = tok_index.reshape(DATA_WAYS, EXPERT_WAYS, E_LOCAL, C_LOCAL).transpose(1, 2, 0, 3)
    return tok_index.reshape(EXPERTS, CAPACITY).astype(jnp.int32)


def setup_inputs(seed: int = 0, part: int = 0) -> dict:
    base_key = jax.random.key(seed)
    part_key = jax.random.fold_in(base_key, part)
    key_x, key_sel, key_gate = jax.random.split(part_key, 3)
    key_in, key_out = jax.random.split(jax.random.key(seed + 1), 2)
    x_tokens = jax.random.normal(key_x, (TOKENS, D_MODEL), jnp.float32).astype(jnp.bfloat16)
    sel_tokens = draw_routes(key_sel)
    gate_w = jax.random.uniform(key_gate, (EXPERTS, CAPACITY), jnp.float32, 0.25, 1.75)
    w_in = (jax.random.normal(key_in, (EXPERTS, D_MODEL, FF_DIM), jnp.float32) * D_MODEL ** -0.5).astype(jnp.bfloat16)
    w_out = (jax.random.normal(key_out, (EXPERTS, FF_DIM, D_MODEL), jnp.float32) * FF_DIM ** -0.5).astype(jnp.bfloat16)
    return {"x_tokens": x_tokens, "sel_tokens": sel_tokens, "gate_w": gate_w, "w_in": w_in, "w_out": w_out}


def reference(x_tokens, sel_tokens, gate_w, w_in, w_out):
    def one_expert(operands):
        sel_row, gate_row, w_first, w_second = operands
        rows = jnp.take(x_tokens, sel_row, axis=0)
        hidden = jnp.dot(rows, w_first, preferred_element_type=jnp.float32)
        hidden = jax.nn.gelu(hidden, approximate=True).astype(jnp.bfloat16)
        expert_out = jnp.dot(hidden, w_second, preferred_element_type=jnp.float32)
        return (gate_row[:, None] * expert_out).astype(jnp.bfloat16)

    contrib = lax.map(one_expert, (sel_tokens, gate_w, w_in, w_out))
    total = jax.ops.segment_sum(contrib.reshape(-1, D_MODEL).astype(jnp.float32), sel_tokens.reshape(-1), num_segments=TOKENS)
    return (x_tokens.astype(jnp.float32) + total).astype(jnp.bfloat16)
```

```python
import functools

import jax
import jax.numpy as jnp
from jax import lax
from jax.experimental import pallas as pl
from jax.experimental.pallas import tpu as pltpu
from jax.sharding import PartitionSpec as P

MESH = pl.DeviceIdType.MESH
VM = pl.BlockSpec(memory_space=pltpu.VMEM)
SM = pl.BlockSpec(memory_space=pltpu.SMEM)
ANY = pl.BlockSpec(memory_space=pl.ANY)
F32, BF16, I32 = jnp.float32, jnp.bfloat16, jnp.int32


def coords():
    return lax.axis_index("pod"), lax.axis_index("data"), lax.axis_index("expert")


def meet(peers):
    barrier = pltpu.get_barrier_semaphore()
    for peer in peers:
        pl.semaphore_signal(barrier, inc=1, device_id=peer, device_id_type=MESH)
    pl.semaphore_wait(barrier, len(peers))


def share_kernel(sel_ref, gate_ref, sel_all, gate_two, send, recv, gsem):
    pod, i, j = coords()
    peers = [(pod, lax.rem(i + di, 2), lax.rem(j + dj, 4)) for di in range(2) for dj in range(4) if (di, dj) != (0, 0)]
    meet(peers)
    me = i * 4 + j
    sel_all[me] = sel_ref[...]
    gate_two[i] = gate_ref[...]
    copies = []
    for k, peer in enumerate(peers):
        copies.append(pltpu.make_async_remote_copy(sel_ref, sel_all.at[me], send.at[k], recv.at[k], device_id=peer, device_id_type=MESH))
    copies.append(pltpu.make_async_remote_copy(gate_ref, gate_two.at[i], gsem.at[0], gsem.at[1], device_id=(pod, 1 - i, j), device_id_type=MESH))
    for c in copies:
        c.start()
    for c in copies:
        c.wait()


def share(sel, gate):
    e, c = sel.shape
    return pl.pallas_call(
        share_kernel,
        out_shape=(jax.ShapeDtypeStruct((8, e, c), I32), jax.ShapeDtypeStruct((2, e, c), F32)),
        in_specs=[VM, VM],
        out_specs=(VM, VM),
        scratch_shapes=[pltpu.SemaphoreType.DMA((7,)), pltpu.SemaphoreType.DMA((7,)), pltpu.SemaphoreType.DMA((2,))],
        compiler_params=pltpu.CompilerParams(collective_id=0, has_side_effects=True),
        name="share",
    )(sel, gate)


def route_kernel(cap_r, sel_all, gate_two, src_ref, xpos_ref, own_ref, part_ref, xrow_ref, gate_ref):
    _, i, j = coords()
    sel = jnp.concatenate([sel_all[j], sel_all[4 + j]], axis=1)
    gate = jnp.concatenate([gate_two[0], gate_two[1]], axis=1)
    half = sel // 4096
    tdev = (sel // 1024) % 4
    row = sel % 1024
    mine = half == i
    src = jnp.where(tdev == j, row, jnp.where(tdev == (j ^ 1), 1024 + row, 2048 + (tdev % 2) * 1024 + row))
    src_ref[...] = jnp.where(mine, src, 0)
    own_ref[...] = jnp.where(mine & (tdev == j), row, -1)
    part_ref[...] = jnp.where(mine & (tdev == (j ^ 1)), row, -1)
    cross = mine & ((tdev // 2) != (j // 2))
    ind = jnp.where(cross, 1.0, 0.0).astype(F32)
    upper = jnp.where(lax.broadcasted_iota(I32, (256, 256), 0) < lax.broadcasted_iota(I32, (256, 256), 1), 1.0, 0.0).astype(BF16)
    within = jnp.dot(ind.astype(BF16), upper, preferred_element_type=F32)
    count = jnp.sum(ind, axis=1, keepdims=True)
    base = jnp.zeros((1, 1), F32)
    rows = []
    for e in range(8):
        rows.append(base)
        base = base + count[e:e + 1]
    xpos = jnp.where(cross, (within + jnp.concatenate(rows, axis=0)).astype(I32), -1)
    xpos_ref[...] = xpos
    xpos_t = jnp.transpose(xpos.astype(F32)).astype(I32)
    tok_t = jnp.transpose(((tdev % 2) * 1024 + row + 1).astype(F32)).astype(I32)
    gate_ref[...] = jnp.transpose(gate)
    lane = lax.broadcasted_iota(I32, (256, cap_r), 1)
    acc = jnp.zeros((1, cap_r), I32)
    for e in range(8):
        acc = acc + jnp.sum(jnp.where(xpos_t[:, e:e + 1] == lane, tok_t[:, e:e + 1], 0), axis=0, keepdims=True)
    xrow_ref[...] = acc - 1


def route(cap_r, sel_all, gate_two):
    slot = jax.ShapeDtypeStruct((8, 256), I32)
    return pl.pallas_call(
        functools.partial(route_kernel, cap_r),
        out_shape=(slot, slot, slot, slot, jax.ShapeDtypeStruct((1, cap_r), I32), jax.ShapeDtypeStruct((256, 8), F32)),
        in_specs=[VM, VM],
        out_specs=(VM,) * 6,
        name="route",
    )(sel_all, gate_two)


def gather_kernel(chunks, x_ref, part_ref, list_ref, psem, ssem, rsem, fsem, gsem):
    pod, i, j = coords()
    partner, across = (pod, i, j ^ 1), (pod, i, j ^ 2)
    core = lax.rem(j, 2)
    meet([partner, across])
    n = x_ref.shape[0] // chunks
    sends = []
    for k in range(chunks):
        rows = pl.ds(k * n, n)
        c = pltpu.make_async_remote_copy(x_ref.at[rows], list_ref.at[core, rows], ssem.at[k], rsem.at[k], device_id=across, device_id_type=MESH)
        c.start()
        sends.append(c)
    pcopy = pltpu.make_async_remote_copy(x_ref, part_ref, psem.at[0], psem.at[1], device_id=partner, device_id_type=MESH)
    pcopy.start()
    forwards = []
    for k in range(chunks):
        rows = pl.ds(k * n, n)
        sends[k].wait_recv()
        f = pltpu.make_async_remote_copy(list_ref.at[core, rows], list_ref.at[core, rows], fsem.at[k], gsem.at[k], device_id=partner, device_id_type=MESH)
        f.start()
        forwards.append(f)
    pcopy.wait()
    for k in range(chunks):
        sends[k].wait_send()
        forwards[k].wait()


def gather(x, chunks=8):
    n, d = x.shape
    return pl.pallas_call(
        functools.partial(gather_kernel, chunks),
        out_shape=(jax.ShapeDtypeStruct((n, d), BF16), jax.ShapeDtypeStruct((2, n, d), BF16)),
        in_specs=[ANY],
        out_specs=(ANY, ANY),
        scratch_shapes=[pltpu.SemaphoreType.DMA((2,))] + [pltpu.SemaphoreType.DMA((chunks,))] * 4,
        compiler_params=pltpu.CompilerParams(collective_id=1, has_side_effects=True),
        name="gather",
    )(x)


def gelu(v):
    return 0.5 * v * (1.0 + jnp.tanh(0.7978845608028654 * (v + 0.044715 * (v * v * v))))


def ffn_kernel(src_ref, x_ref, part_ref, list_ref, gate_ref, win_ref, wout_ref, q_ref, stage, table, rows32, rows16, acc, sem):
    e, f = pl.program_id(0), pl.program_id(1)

    @pl.when((e == 0) & (f == 0))
    def _():
        copies = []
        for k, ref in enumerate((x_ref, part_ref, list_ref.at[0], list_ref.at[1])):
            c = pltpu.make_async_copy(ref, stage.at[k], sem.at[k])
            c.start()
            copies.append(c)
        for k in range(4):
            copies[k].wait()

            @pl.loop(0, 1024 // 128)
            def _(b):
                for s in range(8):
                    piece = stage[k, pl.ds(b * 128, 128), s * 128:(s + 1) * 128].astype(F32)
                    table[pl.ds((k * 1024 + b * 128) * 8 + s, 128, 8), :] = piece

    @pl.when(f == 0)
    def _():
        @pl.loop(0, 256 // 16)
        def _(b):
            for u in range(16):
                r = b * 16 + u
                idx = src_ref[e, r]
                rows32[pl.ds(pl.multiple_of(r * 8, 8), 8), :] = table[pl.ds(pl.multiple_of(idx * 8, 8), 8), :]

        for s in range(8):
            rows16[:, s * 128:(s + 1) * 128] = rows32[pl.ds(s, 256, 8), :].astype(BF16)

    hidden = jnp.dot(rows16[...], win_ref[0], preferred_element_type=F32)
    hidden = gelu(hidden).astype(BF16)
    out = jnp.dot(hidden, wout_ref[0], preferred_element_type=F32)

    @pl.when(f == 0)
    def _():
        acc[...] = out

    @pl.when(f > 0)
    def _():
        acc[...] += out

    @pl.when(f == pl.num_programs(1) - 1)
    def _():
        cols = gate_ref[...]
        lane = lax.broadcasted_iota(I32, cols.shape, 1)
        g = jnp.sum(jnp.where(lane == e, cols, 0.0), axis=1, keepdims=True)
        q_ref[0] = (g * acc[...]).astype(BF16)


def ffn(src, x, part, lists, gate_t, w_in, w_out, tile=1024):
    e, d, ff = w_in.shape
    return pl.pallas_call(
        ffn_kernel,
        out_shape=jax.ShapeDtypeStruct((e, 256, d), BF16),
        grid=(e, ff // tile),
        in_specs=[SM, ANY, ANY, ANY, VM,
                  pl.BlockSpec((1, d, tile), lambda a, b: (a, 0, b)),
                  pl.BlockSpec((1, tile, d), lambda a, b: (a, b, 0))],
        out_specs=pl.BlockSpec((1, 256, d), lambda a, b: (a, 0, 0)),
        scratch_shapes=[pltpu.VMEM((4, 1024, d), BF16), pltpu.VMEM((4096 * 8, 128), F32), pltpu.VMEM((256 * 8, 128), F32),
                        pltpu.VMEM((256, d), BF16), pltpu.VMEM((256, d), F32), pltpu.SemaphoreType.DMA((4,))],
        compiler_params=pltpu.CompilerParams(dimension_semantics=("arbitrary", "arbitrary"), vmem_limit_bytes=56 * 2**20),
        cost_estimate=pl.CostEstimate(flops=4 * e * 256 * d * ff, bytes_accessed=4 * e * d * ff, transcendentals=0),
        name="ffn",
    )(src, x, part, lists, gate_t, w_in, w_out)


def one_hot(index_row, n):
    return jnp.where(lax.broadcasted_iota(I32, (n, index_row.shape[1]), 0) == index_row, 1.0, 0.0).astype(BF16)


def combine_kernel(cap, chunks, x_ref, q_ref, xpos_ref, own_ref, part_ref, xrow_ref, y_ref,
                   total, pq, prow, slist, rlist, xrows, psem, ssem, rsem, fsem, gsem, hsem):
    pod, i, j = coords()
    partner, across = (pod, i, j ^ 1), (pod, i, j ^ 2)
    core = lax.rem(j, 2)
    n = cap // chunks
    meet([partner, across])
    remote = functools.partial(pltpu.make_async_remote_copy, device_id_type=MESH)
    first = [
        remote(part_ref, prow, psem.at[0], psem.at[1], device_id=partner),
        remote(q_ref, pq, psem.at[2], psem.at[3], device_id=partner),
        remote(xrow_ref, xrows.at[0], psem.at[4], psem.at[5], device_id=across),
    ]
    for c in first:
        c.start()

    sends = [remote(slist.at[pl.ds(k * n, n)], rlist.at[0, pl.ds(k * n, n)], ssem.at[k], rsem.at[k], device_id=across) for k in range(chunks)]
    for k in range(chunks):
        @pl.loop(0, 4)
        def _(b):
            cols = pl.ds(pl.multiple_of(b * 256, 256), 256)
            acc = jnp.zeros((n, 256), F32)
            for e in range(8):
                acc = acc + jnp.dot(one_hot(xpos_ref[e:e + 1, :] - k * n, n), q_ref[e, :, cols], preferred_element_type=F32)
            slist[pl.ds(k * n, n), cols] = acc.astype(BF16)
        if k > 0:
            sends[k - 1].start()

    def add(rows, value_of, init=False):
        mats = None

        @pl.loop(0, 4)
        def _(b):
            cols = pl.ds(pl.multiple_of(b * 256, 256), 256)
            acc = x_ref[:, cols].astype(F32) if init else total[:, cols]
            for m, r in enumerate(rows):
                acc = acc + jnp.dot(one_hot(r, 1024), value_of(m, cols), preferred_element_type=F32)
            total[:, cols] = acc

    add([own_ref[e:e + 1, :] for e in range(4)], lambda m, cols: q_ref[m, :, cols], init=True)
    sends[chunks - 1].start()
    add([own_ref[e:e + 1, :] for e in range(4, 8)], lambda m, cols: q_ref[4 + m, :, cols])
    first[0].wait()
    first[1].wait()
    add([prow[e:e + 1, :] for e in range(4)], lambda m, cols: pq[m, :, cols])
    add([prow[e:e + 1, :] for e in range(4, 8)], lambda m, cols: pq[4 + m, :, cols])

    first[2].wait()
    pass_rows = remote(xrows.at[0], xrows.at[1], hsem.at[0], hsem.at[1], device_id=partner)
    pass_rows.start()
    forwards = []
    for k in range(chunks):
        rows = pl.ds(k * n, n)
        sends[k].wait_recv()
        f = remote(rlist.at[0, rows], rlist.at[1, rows], fsem.at[k], gsem.at[k], device_id=partner)
        f.start()
        forwards.append(f)
        add([xrows[0, :, k * n:(k + 1) * n] - core * 1024], lambda m, cols: rlist[0, rows, cols])
    pass_rows.wait()
    for k in range(chunks):
        rows = pl.ds(k * n, n)
        forwards[k].wait()
        add([xrows[1, :, k * n:(k + 1) * n] - core * 1024], lambda m, cols: rlist[1, rows, cols])
    for k in range(chunks):
        sends[k].wait_send()
    y_ref[...] = total[...].astype(BF16)


def combine(x, q, xpos, own, part, xrow, chunks=4):
    n, d = x.shape
    cap = xrow.shape[1]
    return pl.pallas_call(
        functools.partial(combine_kernel, cap, chunks),
        out_shape=jax.ShapeDtypeStruct((n, d), BF16),
        in_specs=[VM] * 6,
        out_specs=VM,
        scratch_shapes=[pltpu.VMEM((n, d), F32), pltpu.VMEM((8, 256, d), BF16), pltpu.VMEM((8, 256), I32),
                        pltpu.VMEM((cap, d), BF16), pltpu.VMEM((2, cap, d), BF16), pltpu.VMEM((2, 1, cap), I32),
                        pltpu.SemaphoreType.DMA((6,))] + [pltpu.SemaphoreType.DMA((chunks,))] * 4 + [pltpu.SemaphoreType.DMA((2,))],
        compiler_params=pltpu.CompilerParams(collective_id=2, has_side_effects=True, vmem_limit_bytes=56 * 2**20),
        name="combine",
    )(x, q, xpos, own, part, xrow)


def solution(mesh):
    row_spec = P(("pod", "data", "expert"), None)
    slot_spec = P(("pod", "expert"), "data")
    weight_spec = P("expert", None, None)

    def local_fn(x, sel, gate, w_in, w_out):
        sel_all, gate_two = share(sel, gate)
        src, xpos, own, part, xrow, gate_t = route(1024, sel_all, gate_two)
        part_x, lists = gather(x)
        q = ffn(src, x, part_x, lists, gate_t, w_in, w_out)
        return combine(x, q, xpos, own, part, xrow)

    return jax.shard_map(local_fn, mesh=mesh, in_specs=(row_spec, slot_spec, slot_spec, weight_spec, weight_spec), out_specs=row_spec, check_vma=False)
```

```python
import functools

import jax
import jax.numpy as jnp
from jax import lax
from jax.experimental import pallas as pl
from jax.experimental.pallas import tpu as pltpu
from jax.sharding import PartitionSpec as P

MESH = pl.DeviceIdType.MESH
VM = pl.BlockSpec(memory_space=pltpu.VMEM)
SM = pl.BlockSpec(memory_space=pltpu.SMEM)
ANY = pl.BlockSpec(memory_space=pl.ANY)
F32, BF16, I32 = jnp.float32, jnp.bfloat16, jnp.int32

LANES, SLOTS, ROWS = 128, 256, 1024
PLANS = ((208, 256, 640, 6, 4), (256, 512, 1024, 3, 4))


def coords():
    return lax.axis_index("pod"), lax.axis_index("data"), lax.axis_index("expert")


def meet(peers):
    barrier = pltpu.get_barrier_semaphore()
    for peer in peers:
        pl.semaphore_signal(barrier, inc=1, device_id=peer, device_id_type=MESH)
    pl.semaphore_wait(barrier, len(peers))


def iota(shape, axis):
    return lax.broadcasted_iota(I32, shape, axis)


def where01(mask):
    return jnp.where(mask, 1.0, 0.0).astype(F32)


def share_kernel(sel_ref, gate_ref, sel_all, gate_two, send, recv, gsem):
    pod, i, j = coords()
    peers = [(pod, lax.rem(i + di, 2), lax.rem(j + dj, 4)) for di in range(2) for dj in range(4) if (di, dj) != (0, 0)]
    meet(peers)
    me = i * 4 + j
    sel_all[me] = sel_ref[...]
    gate_two[i] = gate_ref[...]
    copies = []
    for k, peer in enumerate(peers):
        copies.append(pltpu.make_async_remote_copy(sel_ref, sel_all.at[me], send.at[k], recv.at[k], device_id=peer, device_id_type=MESH))
    copies.append(pltpu.make_async_remote_copy(gate_ref, gate_two.at[i], gsem.at[0], gsem.at[1], device_id=(pod, 1 - i, j), device_id_type=MESH))
    for c in copies:
        c.start()
    for c in copies:
        c.wait()


def share(sel, gate):
    e, c = sel.shape
    return pl.pallas_call(
        share_kernel,
        out_shape=(jax.ShapeDtypeStruct((8, e, c), I32), jax.ShapeDtypeStruct((2, e, c), F32)),
        in_specs=[VM, VM],
        out_specs=(VM, VM),
        scratch_shapes=[pltpu.SemaphoreType.DMA((7,)), pltpu.SemaphoreType.DMA((7,)), pltpu.SemaphoreType.DMA((2,))],
        compiler_params=pltpu.CompilerParams(collective_id=0, has_side_effects=True),
        name="share",
    )(sel, gate)


def route_kernel(sel_all, gate_two, tok_ref, place_ref, lrow_ref, flag_ref, gate_ref, xpos_ref, own_ref, part_ref, xrow_ref, pos_scr):
    _, i, j = coords()
    chip = j // 2

    pos, tot = [], []
    for X in range(2):
        his, los = [], []
        for d in (2 * X, 2 * X + 1, 4 + 2 * X, 5 + 2 * X):
            for e in range(8):
                r = sel_all[d, e:e + 1, :]
                his.append(where01(iota((64, LANES), 0) == r // LANES).astype(BF16))
                los.append(where01(iota((LANES, LANES), 0) == r % LANES).astype(BF16))
        hi = jnp.concatenate(his, axis=1)
        lo = jnp.concatenate(los, axis=1)
        counts = lax.dot_general(hi, lo, (((1,), (1,)), ((), ())), preferred_element_type=F32)
        need = where01(counts > 0.5)
        upper = where01(iota((LANES, LANES), 0) < iota((LANES, LANES), 1)).astype(BF16)
        r64, c64 = iota((64, 64), 0), iota((64, 64), 1)
        lower = where01((c64 < r64) & (c64 // 8 == r64 // 8)).astype(BF16)
        need16 = need.astype(BF16)
        before = jnp.dot(need16, upper, preferred_element_type=F32)
        offset = jnp.sum(jnp.dot(lower, need16, preferred_element_type=F32), axis=1, keepdims=True)
        pos.append(jnp.where(need > 0.5, before + offset, -1.0).astype(I32))
        per_dev = jnp.sum(jnp.dot(where01(iota((8, 64), 0) == iota((8, 64), 1) // 8).astype(BF16), need16, preferred_element_type=F32), axis=1, keepdims=True)
        dev = iota((8, 1), 0)
        tot.append(jnp.where((dev % 4) // 2 != X, per_dev, 0.0))
    longest = jnp.max(jnp.maximum(tot[0], tot[1]))

    pos_scr[...] = jnp.where(chip == 0, pos[0], pos[1])
    mine_pos = pos_scr[pl.ds(pl.multiple_of(i * 32, 32), 32), :]
    block = iota((32, LANES), 0)
    tdev = block // 8
    row = (block % 8) * LANES + iota((32, LANES), 1)
    place_ref[...] = jnp.where(tdev == j, row, jnp.where(tdev == (j ^ 1), ROWS + row, 2048 + (tdev % 2) * ROWS + jnp.maximum(mine_pos, 0)))

    pos_scr[...] = jnp.where(chip == 0, pos[1], pos[0])
    out_pos = pos_scr[pl.ds(pl.multiple_of((i * 4 + j) * 8, 8), 8), :]
    out_t = jnp.transpose(out_pos.astype(F32)).astype(I32)
    lane = iota((LANES, ROWS), 1)
    acc = jnp.zeros((LANES, ROWS), I32)
    for h in range(8):
        acc = acc + jnp.where(out_t[:, h:h + 1] == lane, iota((LANES, 1), 0) + h * LANES, 0)
    lrow_ref[...] = jnp.sum(acc, axis=0, keepdims=True)

    sel = jnp.concatenate([sel_all[j], sel_all[4 + j]], axis=1)
    gate = jnp.concatenate([gate_two[0], gate_two[1]], axis=1)
    tdev = (sel // ROWS) % 4
    row = sel % ROWS
    mine = (sel // 4096) == i
    cross = mine & ((tdev // 2) != chip)
    upper = where01(iota((SLOTS, SLOTS), 0) < iota((SLOTS, SLOTS), 1)).astype(BF16)
    rank = jnp.dot(where01(mine).astype(BF16), upper, preferred_element_type=F32).astype(I32)
    rank = jnp.where(mine, rank, -1)
    amount = jnp.sum(where01(mine), axis=1, keepdims=True)
    xrank = jnp.dot(where01(cross).astype(BF16), upper, preferred_element_type=F32)
    xamount = jnp.sum(where01(cross), axis=1, keepdims=True)
    odd = (iota((8, 8), 0) == iota((8, 8), 1) + 1) & (iota((8, 8), 0) % 2 == 1)
    xbase = jnp.concatenate([jnp.zeros((1, 1), F32), xamount[:7]], axis=0)
    xbase = jnp.where(iota((8, 1), 0) % 2 == 1, xbase, 0.0)
    xpos = jnp.where(cross, (xrank + xbase).astype(I32), -1)
    packed = (sel % 4096) + 4096 * (xpos + 1)
    rank_t = jnp.transpose(rank.astype(F32)).astype(I32)
    packed_t = jnp.transpose(packed.astype(F32)).astype(I32)
    xpos_t = jnp.transpose(xpos.astype(F32)).astype(I32)
    far_t = jnp.transpose(((tdev % 2) * ROWS + row + 1).astype(F32)).astype(I32)
    lane = iota((SLOTS, SLOTS), 1)
    toks, columns = [], []
    for e in range(8):
        toks.append(jnp.sum(jnp.where(rank_t[:, e:e + 1] == lane, packed_t[:, e:e + 1], 0), axis=0, keepdims=True))
        gate_ref[:, e:e + 1] = jnp.sum(jnp.where(rank[e:e + 1, :] == iota((SLOTS, SLOTS), 0), gate[e:e + 1, :], 0.0), axis=1, keepdims=True)
    table = jnp.concatenate(toks, axis=0)
    tok = table % 4096
    tok_ref[...] = tok
    xpos_ref[...] = table // 4096 - 1
    there = iota((8, SLOTS), 1).astype(F32) < amount
    tdev = tok // ROWS
    own_ref[...] = jnp.where(there & (tdev == j), tok % ROWS, -1)
    part_ref[...] = jnp.where(there & (tdev == (j ^ 1)), tok % ROWS, -1)
    lane = iota((SLOTS, 512), 1)
    for g in range(4):
        acc = jnp.zeros((SLOTS, 512), I32)
        for e in (2 * g, 2 * g + 1):
            acc = acc + jnp.where(xpos_t[:, e:e + 1] == lane, far_t[:, e:e + 1], 0)
        xrow_ref[g:g + 1, :] = jnp.sum(acc, axis=0, keepdims=True) - 1

    most = jnp.zeros((8, 1), F32)
    xmost = jnp.zeros((8, 1), F32)
    for jj in range(4):
        s = jnp.concatenate([sel_all[jj], sel_all[4 + jj]], axis=1)
        far = ((s // ROWS) % 4) // 2 != jj // 2
        for h in range(2):
            m = (s // 4096) == h
            most = jnp.maximum(most, jnp.sum(where01(m), axis=1, keepdims=True))
            x = jnp.sum(where01(m & far), axis=1, keepdims=True)
            nxt = jnp.concatenate([x[1:], jnp.zeros((1, 1), F32)], axis=0)
            xmost = jnp.maximum(xmost, jnp.where(iota((8, 1), 0) % 2 == 0, x + nxt, 0.0))
    most = jnp.max(most)
    xmost = jnp.max(xmost)
    plan = jnp.int32(len(PLANS) - 1)
    for p in reversed(range(len(PLANS) - 1)):
        m, c, g = PLANS[p][:3]
        plan = jnp.where((most <= m) & (xmost <= c) & (longest <= g), p, plan)
    flag_ref[0, 0] = plan


def route(sel_all, gate_two):
    slot = jax.ShapeDtypeStruct((8, SLOTS), I32)
    return pl.pallas_call(
        route_kernel,
        out_shape=(slot, jax.ShapeDtypeStruct((32, LANES), I32), jax.ShapeDtypeStruct((1, ROWS), I32), jax.ShapeDtypeStruct((1, 1), I32),
                   jax.ShapeDtypeStruct((SLOTS, 8), F32), slot, slot, slot, jax.ShapeDtypeStruct((4, 512), I32)),
        in_specs=[VM, VM],
        out_specs=(VM, VM, VM, SM, VM, VM, VM, VM, VM),
        scratch_shapes=[pltpu.VMEM((64, LANES), I32)],
        name="route",
    )(sel_all, gate_two)


def gelu(v):
    return (0.5 * v) * (1.0 + jnp.tanh(v * (0.7978845608028654 + 0.035677408136300125 * (v * v))))


def layer_kernel(plan, tok_ref, place_ref, lrow_ref, x_ref, gate_ref, xpos_ref, own_ref, part_ref, xrow_ref, win_ref, wout_ref, y_ref,
                 xown, table, slist, rows32, tmp32, rows16, hid, acc, qq, total, rsend, rlist, prow, xrows, wi, wo, amat, src,
                 wsem, psem, lsem, qsem, rsem):
    M, cap, cap_g, depth, pieces = plan
    pod, i, j = coords()
    partner, across = (pod, i, j ^ 1), (pod, i, j ^ 2)
    core = lax.rem(j, 2)
    remote = functools.partial(pltpu.make_async_remote_copy, device_id_type=MESH)
    F = ROWS
    steps = 32

    def weights(k, slot):
        e, f = k // 4, lax.rem(k, 4)
        cols = pl.ds(pl.multiple_of(f * F, F), F)
        return (pltpu.make_async_copy(win_ref.at[e, :, cols], wi.at[slot], wsem.at[0, slot]),
                pltpu.make_async_copy(wout_ref.at[e, cols, :], wo.at[slot], wsem.at[1, slot]))

    @pl.loop(0, depth)
    def _(k):
        for c in weights(k, k):
            c.start()

    meet([partner, across])
    small = [remote(part_ref, prow, psem.at[0], psem.at[1], device_id=partner),
             remote(xrow_ref, xrows.at[core], psem.at[2], psem.at[3], device_id=across)]
    for c in small:
        c.start()

    @pl.loop(0, 8)
    def _(b):
        at = pl.multiple_of(b * LANES, LANES)
        for s in range(8):
            tmp32[pl.ds(s, LANES, 8), :] = x_ref[pl.ds(at, LANES), s * LANES:(s + 1) * LANES].astype(F32)
        tiles = tmp32[...].reshape(LANES, 8, LANES).astype(BF16)
        xown[pl.ds(at, LANES)] = tiles
        table[pl.ds(at, LANES)] = tiles

    pcopy = remote(xown, table.at[pl.ds(ROWS, ROWS)], psem.at[4], psem.at[5], device_id=partner)
    n = cap_g // pieces
    base = 2048 + core * ROWS
    sends, forwards = [], []
    for k in range(pieces):
        there = table.at[pl.ds(base + k * n, n)]
        sends.append(remote(slist.at[pl.ds(k * n, n)], there, lsem.at[0, k], lsem.at[1, k], device_id=across))
        forwards.append(remote(there, there, lsem.at[2, k], lsem.at[3, k], device_id=partner))
    for k in range(pieces):
        @pl.loop(0, n // 16)
        def _(b):
            tiles = [xown[lrow_ref[0, k * n + b * 16 + u]] for u in range(16)]
            for u, tile in enumerate(tiles):
                slist[k * n + b * 16 + u] = tile

        if k == 0:
            pcopy.start()
        else:
            sends[k - 1].start()
    total[...] = x_ref[...].astype(F32)
    sends[pieces - 1].start()
    @pl.loop(0, 8)
    def _(e):
        @pl.loop(0, M // 16)
        def _(b):
            for u in range(16):
                tok = tok_ref[e, b * 16 + u]
                src[e, b * 16 + u] = place_ref[tok >> 7, tok & (LANES - 1)]

    small[1].wait()
    pass_rows = remote(xrows.at[core], xrows.at[core], psem.at[6], psem.at[7], device_id=partner)
    pass_rows.start()
    for k in range(pieces):
        sends[k].wait_recv()
        forwards[k].start()
    small[0].wait()
    pass_rows.wait()
    pcopy.wait()
    for k in range(pieces):
        sends[k].wait_send()
        forwards[k].wait()

    def fetch(e, slot, f):
        at = pl.multiple_of(jnp.minimum(f * 64, M - 64), 16)
        for v in range(0, 64, 16):
            tiles = [table[src[e, at + v + u]].astype(F32) for u in range(16)]
            for u, tile in enumerate(tiles):
                rows32[(v + u) * 8:(v + u + 1) * 8, :] = tile
        for s in range(8):
            rows16[slot, pl.ds(at, 64), s * LANES:(s + 1) * LANES] = rows32[pl.ds(s, 64, 8), :].astype(BF16)

    @pl.loop(0, 4)
    def _(f):
        fetch(0, 0, f)

    def qcopy(g):
        return remote(qq.at[g, pl.ds(0, 2 * M)], qq.at[g, pl.ds(2 * M, 2 * M)], qsem.at[0, g], qsem.at[1, g], device_id=partner)

    def xcopy(g):
        return remote(rsend.at[g], rlist.at[g, pl.ds(core * cap, cap)], rsem.at[0, g], rsem.at[1, g], device_id=across)

    def xpass(g):
        there = rlist.at[g, pl.ds(core * cap, cap)]
        return remote(there, there, rsem.at[2, g], rsem.at[3, g], device_id=partner)

    def pair(ref, g):
        return jnp.concatenate([ref[pl.ds(2 * g, 1), :][:, :M], ref[pl.ds(2 * g + 1, 1), :][:, :M]], axis=1)

    def add(rows, ref, g):
        k = rows.shape[1]
        for b in range(4):
            amat[b * SLOTS:(b + 1) * SLOTS, :k] = where01(iota((SLOTS, k), 0) + b * SLOTS == rows).astype(BF16)

        @pl.loop(0, 4)
        def _(b):
            cols = pl.ds(pl.multiple_of(b * SLOTS, SLOTS), SLOTS)
            total[:, cols] += jnp.dot(amat[:, :k], ref[g, :, cols], preferred_element_type=F32)

    def add_chip(g):
        qcopy(g).wait_recv()
        add(jnp.concatenate([pair(own_ref, g), pair(prow, g)], axis=1), qq, g)

    def take_far(g):
        xcopy(g).wait_recv()
        xpass(g).start()

    def add_far(g):
        xpass(g).wait_recv()
        add(jnp.concatenate([xrows[0, pl.ds(g, 1), :][:, :cap], xrows[1, pl.ds(g, 1), :][:, :cap]], axis=1) - core * ROWS, rlist, g)

    @pl.loop(0, 4)
    def _(g):
        @pl.loop(0, 8)
        def _(t):
            k = g * 8 + t
            e = k // 4
            f = lax.rem(k, 4)
            cur = lax.rem(e, 2)
            slot = lax.rem(k, depth)
            for c in weights(k, slot):
                c.wait()
            fetch(jnp.minimum(e + 1, 7), 1 - cur, f)
            xs = rows16[cur]
            for s in range(4):
                u = jnp.dot(xs, wi[slot, :, s * SLOTS:(s + 1) * SLOTS], preferred_element_type=F32)
                hid[:, s * SLOTS:(s + 1) * SLOTS] = gelu(u).astype(BF16)
            out = jnp.dot(hid[...], wo[slot], preferred_element_type=F32)
            acc[...] = jnp.where(f == 0, out, acc[...] + out)

            @pl.when(k + depth < steps)
            def _():
                for c in weights(k + depth, slot):
                    c.start()

            @pl.when(f == 3)
            def _():
                cols = gate_ref[...]
                weight = jnp.sum(jnp.where(iota(cols.shape, 1) == e, cols, 0.0), axis=1, keepdims=True)[:M]
                qq[g, pl.ds(pl.multiple_of(cur * M, 16), M), :] = (weight * acc[...]).astype(BF16)

        amat[:cap, :2 * M] = where01(iota((cap, 2 * M), 0) == pair(xpos_ref, g)).astype(BF16)

        @pl.loop(0, 4)
        def _(b):
            cols = pl.ds(pl.multiple_of(b * SLOTS, SLOTS), SLOTS)
            rsend[g, :, cols] = jnp.dot(amat[:cap, :2 * M], qq[g, :2 * M, cols], preferred_element_type=F32).astype(BF16)

        qcopy(g).start()

        @pl.when(g >= 2)
        def _():
            take_far(g - 2)

        @pl.when(g == 0)
        def _():
            xcopy(g).start()

        @pl.when(g >= 1)
        def _():
            k = 4 * M
            rows = jnp.concatenate([pair(own_ref, g - 1), pair(prow, g - 1)], axis=1)
            for b in range(4):
                amat[b * SLOTS:(b + 1) * SLOTS, :k] = where01(iota((SLOTS, k), 0) + b * SLOTS == rows).astype(BF16)
            xcopy(g).start()
            qcopy(g - 1).wait_recv()

            @pl.loop(0, 4)
            def _(b):
                cols = pl.ds(pl.multiple_of(b * SLOTS, SLOTS), SLOTS)
                total[:, cols] += jnp.dot(amat[:, :k], qq[g - 1, :, cols], preferred_element_type=F32)

        @pl.when(g >= 3)
        def _():
            add_far(g - 3)

    take_far(2)
    add_chip(3)
    add_far(1)
    add_far(2)
    take_far(3)
    add_far(3)
    for g in range(4):
        qcopy(g).wait_send()
        xcopy(g).wait_send()
        xpass(g).wait_send()
    y_ref[...] = total[...].astype(BF16)


def layer(index, tok, place, lrow, x, gate_t, xpos, own, part, xrow, w_in, w_out):
    plan = PLANS[index]
    M, cap, cap_g, depth, pieces = plan
    n, d = x.shape
    e, _, ff = w_in.shape
    dma = pltpu.SemaphoreType.DMA
    return pl.pallas_call(
        functools.partial(layer_kernel, plan),
        out_shape=jax.ShapeDtypeStruct((n, d), BF16),
        in_specs=[SM, SM, SM, VM, VM, VM, VM, VM, VM, ANY, ANY],
        out_specs=VM,
        scratch_shapes=[pltpu.VMEM((n, 8, LANES), BF16), pltpu.VMEM((3072 + cap_g, 8, LANES), BF16), pltpu.VMEM((cap_g, 8, LANES), BF16),
                        pltpu.VMEM((64 * 8, LANES), F32), pltpu.VMEM((LANES * 8, LANES), F32), pltpu.VMEM((2, M, d), BF16),
                        pltpu.VMEM((M, ROWS), BF16), pltpu.VMEM((M, d), F32), pltpu.VMEM((4, 4 * M, d), BF16), pltpu.VMEM((n, d), F32),
                        pltpu.VMEM((4, cap, d), BF16), pltpu.VMEM((4, 2 * cap, d), BF16), pltpu.VMEM((8, SLOTS), I32), pltpu.VMEM((2, 4, 512), I32),
                        pltpu.VMEM((depth, d, ROWS), BF16), pltpu.VMEM((depth, ROWS, d), BF16), pltpu.VMEM((n, max(4 * M, 2 * cap)), BF16), pltpu.SMEM((8, SLOTS), I32),
                        dma((2, depth)), dma((8,)), dma((4, pieces)), dma((2, 4)), dma((4, 4))],
        compiler_params=pltpu.CompilerParams(collective_id=1 + index, has_side_effects=True, vmem_limit_bytes=67043328),
        cost_estimate=pl.CostEstimate(flops=4 * e * M * d * ff, bytes_accessed=4 * e * d * ff, transcendentals=0),
        name="layer%d" % index,
    )(tok, place, lrow, x, gate_t, xpos, own, part, xrow, w_in, w_out)


def solution(mesh):
    row_spec = P(("pod", "data", "expert"), None)
    slot_spec = P(("pod", "expert"), "data")
    weight_spec = P("expert", None, None)

    def local_fn(x, sel, gate, w_in, w_out):
        sel_all, gate_two = share(sel, gate)
        tok, place, lrow, flag, gate_t, xpos, own, part, xrow = route(sel_all, gate_two)
        args = (tok, place, lrow, x, gate_t, xpos, own, part, xrow, w_in, w_out)
        return lax.switch(flag[0, 0], [functools.partial(layer, k) for k in range(len(PLANS))], *args)

    return jax.shard_map(local_fn, mesh=mesh, in_specs=(row_spec, slot_spec, slot_spec, weight_spec, weight_spec), out_specs=row_spec, check_vma=False)
```

```python
import functools

import jax
import jax.numpy as jnp
from jax import lax
from jax.experimental import pallas as pl
from jax.experimental.pallas import tpu as pltpu
from jax.sharding import PartitionSpec as P

MESH = pl.DeviceIdType.MESH
VM = pl.BlockSpec(memory_space=pltpu.VMEM)
SM = pl.BlockSpec(memory_space=pltpu.SMEM)
ANY = pl.BlockSpec(memory_space=pl.ANY)
F32, BF16, I32 = jnp.float32, jnp.bfloat16, jnp.int32

LANES, SLOTS, ROWS = 128, 256, 1024
STATIC = 256
PLANS = ((208, 80, 128, 480, 7, 4, 2), (256, 256, 256, 768, 3, 4, 1))


def coords():
    return lax.axis_index("pod"), lax.axis_index("data"), lax.axis_index("expert")


def meet(peers):
    barrier = pltpu.get_barrier_semaphore()
    for peer in peers:
        pl.semaphore_signal(barrier, inc=1, device_id=peer, device_id_type=MESH)
    pl.semaphore_wait(barrier, len(peers))


def iota(shape, axis):
    return lax.broadcasted_iota(I32, shape, axis)


def where01(mask):
    return jnp.where(mask, 1.0, 0.0).astype(F32)


def front_kernel(sel_ref, gate_in, x_ref, own3, part3, far3, tok_ref, place_ref, lrow_ref, flag_ref, gate_ref, dpos_ref, rows_ref,
                 sel_all, gate_two, tmp32, xown, pos_scr, send, recv, gsem, csem):
    pod, i, j = coords()
    chip = j // 2
    core = lax.rem(j, 2)
    partner, across = (pod, i, j ^ 1), (pod, i, j ^ 2)
    remote = functools.partial(pltpu.make_async_remote_copy, device_id_type=MESH)
    peers = [(pod, lax.rem(i + di, 2), lax.rem(j + dj, 4)) for di in range(2) for dj in range(4) if (di, dj) != (0, 0)]
    meet(peers)
    me = i * 4 + j
    sel_all[me] = sel_ref[...]
    gate_two[i] = gate_in[...]
    shares = [remote(sel_ref, sel_all.at[me], send.at[k], recv.at[k], device_id=peer) for k, peer in enumerate(peers)]
    shares.append(remote(gate_in, gate_two.at[i], gsem.at[0], gsem.at[1], device_id=(pod, 1 - i, j)))
    for c in shares:
        c.start()

    first = remote(xown.at[pl.ds(0, STATIC)], far3.at[core], csem.at[0], csem.at[1], device_id=across)
    second = remote(far3.at[core], far3.at[core], csem.at[2], csem.at[3], device_id=partner)
    whole = remote(xown, part3, csem.at[4], csem.at[5], device_id=partner)
    keep = pltpu.make_async_copy(xown, own3, csem.at[6])

    @pl.loop(0, ROWS // LANES)
    def _(b):
        at = pl.multiple_of(b * LANES, LANES)
        for s in range(8):
            tmp32[pl.ds(s, LANES, 8), :] = x_ref[pl.ds(at, LANES), s * LANES:(s + 1) * LANES].astype(F32)
        xown[pl.ds(at, LANES)] = tmp32[...].reshape(LANES, 8, LANES).astype(BF16)

        @pl.when(b == STATIC // LANES)
        def _():
            first.start()

    for c in shares:
        c.wait()
    whole.start()
    keep.start()

    pos, tot = [], []
    block = iota((64, LANES), 0)
    late = (block % 8) >= STATIC // LANES
    for X in range(2):
        his, los = [], []
        for d in (2 * X, 2 * X + 1, 4 + 2 * X, 5 + 2 * X):
            for e in range(8):
                r = sel_all[d, e:e + 1, :]
                his.append(where01(block == r // LANES).astype(BF16))
                los.append(where01(iota((LANES, LANES), 0) == r % LANES).astype(BF16))
        hi = jnp.concatenate(his, axis=1)
        lo = jnp.concatenate(los, axis=1)
        counts = lax.dot_general(hi, lo, (((1,), (1,)), ((), ())), preferred_element_type=F32)
        need = where01((counts > 0.5) & late)
        upper = where01(iota((LANES, LANES), 0) < iota((LANES, LANES), 1)).astype(BF16)
        r64, c64 = iota((64, 64), 0), iota((64, 64), 1)
        lower = where01((c64 < r64) & (c64 // 8 == r64 // 8)).astype(BF16)
        need16 = need.astype(BF16)
        before = jnp.dot(need16, upper, preferred_element_type=F32)
        offset = jnp.sum(jnp.dot(lower, need16, preferred_element_type=F32), axis=1, keepdims=True)
        pos.append(jnp.where(need > 0.5, before + offset, -1.0).astype(I32))
        per_dev = jnp.sum(jnp.dot(where01(iota((8, 64), 0) == iota((8, 64), 1) // 8).astype(BF16), need16, preferred_element_type=F32), axis=1, keepdims=True)
        tot.append(jnp.where((iota((8, 1), 0) % 4) // 2 != X, per_dev, 0.0))
    longest = jnp.max(jnp.maximum(tot[0], tot[1]))

    pos_scr[...] = jnp.where(chip == 0, pos[0], pos[1])
    mine_pos = pos_scr[pl.ds(pl.multiple_of(i * 32, 32), 32), :]
    block = iota((32, LANES), 0)
    tdev = block // 8
    row = (block % 8) * LANES + iota((32, LANES), 1)
    other = lax.rem(tdev, 2)
    far_place = 2 * ROWS + jnp.where(row < STATIC, other * STATIC + row, 2 * STATIC + other * (ROWS - STATIC) + jnp.maximum(mine_pos, 0))
    place_ref[...] = jnp.where(tdev == j, row, jnp.where(tdev == (j ^ 1), ROWS + row, far_place))

    pos_scr[...] = jnp.where(chip == 0, pos[1], pos[0])
    out_pos = pos_scr[pl.ds(pl.multiple_of((i * 4 + j) * 8, 8), 8), :]
    out_t = jnp.transpose(out_pos.astype(F32)).astype(I32)
    lane = iota((LANES, ROWS), 1)
    acc = jnp.zeros((LANES, ROWS), I32)
    for h in range(STATIC // LANES, 8):
        acc = acc + jnp.where(out_t[:, h:h + 1] == lane, iota((LANES, 1), 0) + h * LANES, 0)
    lrow_ref[...] = jnp.sum(acc, axis=0, keepdims=True)

    sel = jnp.concatenate([sel_all[j], sel_all[4 + j]], axis=1)
    gate = jnp.concatenate([gate_two[0], gate_two[1]], axis=1)
    tdev = (sel // ROWS) % 4
    row = sel % ROWS
    mine = (sel // (4 * ROWS)) == i
    upper = where01(iota((SLOTS, SLOTS), 0) < iota((SLOTS, SLOTS), 1)).astype(BF16)

    def order(mask):
        return jnp.dot(where01(mask).astype(BF16), upper, preferred_element_type=F32).astype(I32)

    rank = jnp.where(mine, order(mine), -1)
    dpos = jnp.full((8, SLOTS), -1, I32)
    for c, mask in enumerate((tdev == j, tdev == (j ^ 1), (tdev // 2) != chip)):
        mask = mine & mask
        dpos = jnp.where(mask, order(mask) + c * SLOTS, dpos)
    packed = (sel % (4 * ROWS)) + 4 * ROWS * (dpos + 1)
    rank_t = jnp.transpose(rank.astype(F32)).astype(I32)
    packed_t = jnp.transpose(packed.astype(F32)).astype(I32)
    dpos_t = jnp.transpose(dpos.astype(F32)).astype(I32)
    row_t = jnp.transpose(((tdev % 2) * ROWS + row + 1).astype(F32)).astype(I32)
    lane = iota((SLOTS, SLOTS), 1)
    wide = iota((SLOTS, 3 * SLOTS), 1)
    toks = []
    for e in range(8):
        toks.append(jnp.sum(jnp.where(rank_t[:, e:e + 1] == lane, packed_t[:, e:e + 1], 0), axis=0, keepdims=True))
        gate_ref[:, e:e + 1] = jnp.sum(jnp.where(rank[e:e + 1, :] == iota((SLOTS, SLOTS), 0), gate[e:e + 1, :], 0.0), axis=1, keepdims=True)
        rows_ref[e:e + 1, :] = jnp.sum(jnp.where(dpos_t[:, e:e + 1] == wide, row_t[:, e:e + 1], 0), axis=0, keepdims=True) - 1
    table = jnp.concatenate(toks, axis=0)
    tok_ref[...] = table % (4 * ROWS)
    dpos_ref[...] = table // (4 * ROWS) - 1

    most = jnp.zeros((8, 1), F32)
    near = jnp.zeros((8, 1), F32)
    far = jnp.zeros((8, 1), F32)
    for jj in range(4):
        s = jnp.concatenate([sel_all[jj], sel_all[4 + jj]], axis=1)
        for h in range(2):
            n = [jnp.sum(where01(s // ROWS == h * 4 + t), axis=1, keepdims=True) for t in range(4)]
            a, b = (n[:2], n[2:]) if jj < 2 else (n[2:], n[:2])
            near = jnp.maximum(near, jnp.maximum(a[0], a[1]))
            far = jnp.maximum(far, b[0] + b[1])
            most = jnp.maximum(most, a[0] + a[1] + b[0] + b[1])
    most, near, far = jnp.max(most), jnp.max(near), jnp.max(far)
    plan = jnp.int32(len(PLANS) - 1)
    for p in reversed(range(len(PLANS) - 1)):
        m, co, cf, g = PLANS[p][:4]
        plan = jnp.where((most <= m) & (near <= co) & (far <= cf) & (longest <= g), p, plan)
    flag_ref[0, 0] = plan

    first.wait_recv()
    second.start()
    first.wait_send()
    whole.wait()
    keep.wait()
    second.wait()


def front(sel, gate, x):
    e, c = sel.shape
    n, d = x.shape
    slot = jax.ShapeDtypeStruct((8, SLOTS), I32)
    tiles = jax.ShapeDtypeStruct((n, 8, LANES), BF16)
    dma = pltpu.SemaphoreType.DMA
    return pl.pallas_call(
        front_kernel,
        out_shape=(tiles, tiles, jax.ShapeDtypeStruct((2, STATIC, 8, LANES), BF16),
                   slot, jax.ShapeDtypeStruct((32, LANES), I32), jax.ShapeDtypeStruct((1, ROWS), I32), jax.ShapeDtypeStruct((1, 1), I32),
                   jax.ShapeDtypeStruct((SLOTS, 8), F32), slot, jax.ShapeDtypeStruct((8, 3 * SLOTS), I32)),
        in_specs=[VM, VM, VM],
        out_specs=(ANY, ANY, ANY, VM, VM, VM, SM, VM, VM, VM),
        scratch_shapes=[pltpu.VMEM((8, e, c), I32), pltpu.VMEM((2, e, c), F32), pltpu.VMEM((LANES * 8, LANES), F32), pltpu.VMEM((n, 8, LANES), BF16),
                        pltpu.VMEM((64, LANES), I32), dma((7,)), dma((7,)), dma((2,)), dma((7,))],
        compiler_params=pltpu.CompilerParams(collective_id=0, has_side_effects=True),
        name="front",
    )(sel, gate, x)


def gelu(v):
    return (0.5 * v) * (1.0 + jnp.tanh(v * (0.7978845608028654 + 0.035677408136300125 * (v * v))))


def layer_kernel(plan, tok_ref, place_ref, lrow_ref, x_ref, gate_ref, dpos_ref, rows_ref, own3, part3, far3, win_ref, wout_ref, y_ref,
                 xown, table, slist, rows32, rows16, hid0, hid1, acc, value, comb, psend, fsend, total, prow, frow, wi, wo, src,
                 wsem, psem, lsem, csem):
    M, co, cf, cap_g, depth, pieces, many = plan
    width = 2 * co + 2 * cf
    pod, i, j = coords()
    partner, across = (pod, i, j ^ 1), (pod, i, j ^ 2)
    core = lax.rem(j, 2)
    remote = functools.partial(pltpu.make_async_remote_copy, device_id_type=MESH)
    steps = 32

    def columns(k):
        return pl.ds(pl.multiple_of(lax.rem(k, 4) * ROWS, ROWS), ROWS)

    def first_weights(k):
        return pltpu.make_async_copy(win_ref.at[k // 4, :, columns(k)], wi.at[lax.rem(k, depth)], wsem.at[0, lax.rem(k, depth)])

    def second_weights(k):
        return pltpu.make_async_copy(wout_ref.at[k // 4, columns(k), :], wo.at[lax.rem(k, depth)], wsem.at[1, lax.rem(k, depth)])

    load = pltpu.make_async_copy(own3, xown, psem.at[0])
    base = 2 * ROWS + 2 * STATIC
    loads = [pltpu.make_async_copy(own3, table.at[pl.ds(0, ROWS)], psem.at[1]),
             pltpu.make_async_copy(part3, table.at[pl.ds(ROWS, ROWS)], psem.at[2]),
             pltpu.make_async_copy(far3.at[0], table.at[pl.ds(2 * ROWS, STATIC)], psem.at[3]),
             pltpu.make_async_copy(far3.at[1], table.at[pl.ds(2 * ROWS + STATIC, STATIC)], psem.at[4])]
    load.start()
    for c in loads:
        c.start()

    @pl.loop(0, depth)
    def _(k):
        first_weights(k).start()
        second_weights(k).start()

    meet([partner, across])
    small = [remote(rows_ref, prow, psem.at[5], psem.at[6], device_id=partner),
             remote(rows_ref, frow.at[core], psem.at[7], psem.at[8], device_id=across)]
    for c in small:
        c.start()

    n = cap_g // pieces
    base = base + core * (ROWS - STATIC)
    sends, forwards = [], []
    for k in range(pieces):
        there = table.at[pl.ds(base + k * n, n)]
        sends.append(remote(slist.at[pl.ds(k * n, n)], there, lsem.at[0, k], lsem.at[1, k], device_id=across))
        forwards.append(remote(there, there, lsem.at[2, k], lsem.at[3, k], device_id=partner))
    load.wait()
    for k in range(pieces):
        @pl.loop(0, n // 8)
        def _(b):
            at = k * n + b * 8
            tiles = [xown[lrow_ref[0, at + u]] for u in range(8)]
            for u, tile in enumerate(tiles):
                slist[at + u] = tile

        if k > 0:
            sends[k - 1].start()
    total[...] = x_ref[...].astype(F32)
    sends[pieces - 1].start()

    @pl.loop(0, 8)
    def _(e):
        @pl.loop(0, M // 16)
        def _(b):
            for u in range(16):
                tok = tok_ref[e, b * 16 + u]
                src[e, b * 16 + u] = place_ref[tok >> 7, tok & (LANES - 1)]

    small[1].wait()
    pass_rows = remote(frow.at[core], frow.at[core], psem.at[9], psem.at[10], device_id=partner)
    pass_rows.start()
    for k in range(pieces):
        sends[k].wait_recv()
        forwards[k].start()
    small[0].wait()
    pass_rows.wait()
    for c in loads:
        c.wait()
    for k in range(pieces):
        sends[k].wait_send()
        forwards[k].wait()

    def fetch(e, slot, f):
        at = pl.multiple_of(jnp.minimum(f * 64, M - 64), 16)
        for v in range(0, 64, 16):
            tiles = [table[src[e, at + v + u]].astype(F32) for u in range(16)]
            for u, tile in enumerate(tiles):
                rows32[(v + u) * 8:(v + u + 1) * 8, :] = tile
        for s in range(8):
            rows16[slot, pl.ds(at, 64), s * LANES:(s + 1) * LANES] = rows32[pl.ds(s, 64, 8), :].astype(BF16)

    @pl.loop(0, 4)
    def _(f):
        fetch(0, 0, f)

    def near(e):
        slot = lax.rem(e, 4)
        return remote(psend.at[slot], comb.at[pl.ds(e * width + co, co)], csem.at[0, e], csem.at[1, e], device_id=partner)

    def far(e):
        slot = lax.rem(e, 4)
        return remote(fsend.at[slot], comb.at[pl.ds(e * width + 2 * co + core * cf, cf)], csem.at[2, e], csem.at[3, e], device_id=across)

    def passed(e):
        there = comb.at[pl.ds(e * width + 2 * co + core * cf, cf)]
        return remote(there, there, csem.at[4, e], csem.at[5, e], device_id=partner)

    def finish(e):
        cols = gate_ref[...]
        weight = jnp.sum(jnp.where(iota(cols.shape, 1) == e, cols, 0.0), axis=1, keepdims=True)[:M]
        value[...] = (weight * acc[...]).astype(BF16)
        d = dpos_ref[pl.ds(e, 1), :][:, :M]
        kind, rank = d >> 8, d & (SLOTS - 1)
        d = jnp.where(d < 0, -1, rank + jnp.where(kind == 0, 0, jnp.where(kind == 1, co, 2 * co)))
        sort = where01(iota((2 * co + cf, M), 0) == d).astype(BF16)
        slot = lax.rem(e, 4)
        for b in range(4):
            cols = slice(b * SLOTS, (b + 1) * SLOTS)
            lists = jnp.dot(sort, value[:, cols], preferred_element_type=F32).astype(BF16)
            comb[pl.ds(pl.multiple_of(e * width, 16), co), cols] = lists[:co]
            psend[slot, :, cols] = lists[co:2 * co]
            fsend[slot, :, cols] = lists[2 * co:]

    def take(e):
        far(e).wait_recv()
        passed(e).start()

    def add(e):
        rows = []
        for m in range(e, e + many):
            passed(m).wait_recv()
            near(m).wait_recv()
            rows += [rows_ref[m:m + 1, :co], prow[m:m + 1, SLOTS:SLOTS + co],
                     frow[0, m:m + 1, 2 * SLOTS:2 * SLOTS + cf], frow[1, m:m + 1, 2 * SLOTS:2 * SLOTS + cf]]
        rows = jnp.concatenate(rows, axis=1) - core * ROWS

        @pl.loop(0, 2)
        def _(b):
            at = pl.multiple_of(b * 2 * SLOTS, 2 * SLOTS)
            put = where01(iota((2 * SLOTS, many * width), 0) + at == rows).astype(BF16)
            total[pl.ds(at, 2 * SLOTS), :] += jnp.dot(put, comb[e * width:(e + many) * width, :], preferred_element_type=F32)

    def first(k, hid):
        xs = rows16[lax.rem(k // 4, 2)]
        for s in range(4):
            u = jnp.dot(xs, wi[lax.rem(k, depth), :, s * SLOTS:(s + 1) * SLOTS], preferred_element_type=F32)
            hid[:, s * SLOTS:(s + 1) * SLOTS] = gelu(u).astype(BF16)

    def second(k, hid):
        out = jnp.dot(hid[...], wo[lax.rem(k, depth)], preferred_element_type=F32)
        acc[...] = jnp.where(lax.rem(k, 4) == 0, out, acc[...] + out)

    def step(k, new, old):
        e = k // 4
        first_weights(k).wait()

        @pl.when(k != 1)
        def _():
            second_weights(jnp.maximum(k - 1, 0)).wait()

        first(k, new)
        second(jnp.maximum(k - 1, 0), old)
        fetch(jnp.minimum(e + 1, 7), 1 - lax.rem(e, 2), lax.rem(k, 4))

        @pl.when(k + depth < steps)
        def _():
            first_weights(k + depth).start()

        @pl.when((k > 0) & (k - 1 + depth < steps))
        def _():
            second_weights(k - 1 + depth).start()

    @pl.loop(0, steps // 2)
    def _(kk):
        k = 2 * kk
        e = kk // 2
        even = lax.rem(kk, 2) == 0
        step(k, hid0, hid1)

        @pl.when(even & (e >= 1))
        def _():
            @pl.when(e >= 5)
            def _():
                near(e - 5).wait_send()
                far(e - 5).wait_send()

            finish(e - 1)

        @pl.when((~even) & (e >= 4))
        def _():
            take(e - 4)

        step(k + 1, hid1, hid0)

        @pl.when(even & (e >= 1))
        def _():
            far(e - 1).start()
            near(e - 1).start()

        @pl.when(kk == steps // 2 - 1)
        def _():
            for m in range(0, 4, many):
                add(m)

    second_weights(steps - 1).wait()
    second(steps - 1, hid1)
    near(3).wait_send()
    far(3).wait_send()
    finish(7)
    take(4)
    far(7).start()
    near(7).start()
    take(5)
    if many == 1:
        add(4)
        add(5)
    else:
        add(4)
    take(6)
    if many == 1:
        add(6)
    take(7)
    add(8 - many)
    for e in range(8):
        if e >= 4:
            near(e).wait_send()
            far(e).wait_send()
        passed(e).wait_send()
    y_ref[...] = total[...].astype(BF16)


def layer(index, tok, place, lrow, x, gate_t, dpos, rows, own3, part3, far3, w_in, w_out):
    plan = PLANS[index]
    M, co, cf, cap_g, depth, pieces, many = plan
    n, d = x.shape
    e, _, ff = w_in.shape
    dma = pltpu.SemaphoreType.DMA
    vm = pltpu.VMEM
    return pl.pallas_call(
        functools.partial(layer_kernel, plan),
        out_shape=jax.ShapeDtypeStruct((n, d), BF16),
        in_specs=[SM, SM, SM, VM, VM, VM, VM, ANY, ANY, ANY, ANY, ANY],
        out_specs=VM,
        scratch_shapes=[vm((n, 8, LANES), BF16), vm((3 * ROWS + STATIC + cap_g, 8, LANES), BF16), vm((cap_g, 8, LANES), BF16),
                        vm((64 * 8, LANES), F32), vm((2, M, d), BF16), vm((M, ROWS), BF16), vm((M, ROWS), BF16), vm((M, d), F32), vm((M, d), BF16),
                        vm((8 * (2 * co + 2 * cf), d), BF16), vm((4, co, d), BF16), vm((4, cf, d), BF16), vm((n, d), F32),
                        vm((8, 3 * SLOTS), I32), vm((2, 8, 3 * SLOTS), I32), vm((depth, d, ROWS), BF16), vm((depth, ROWS, d), BF16),
                        pltpu.SMEM((8, SLOTS), I32), dma((2, depth)), dma((11,)), dma((4, pieces)), dma((6, 8))],
        compiler_params=pltpu.CompilerParams(collective_id=1 + index, has_side_effects=True, vmem_limit_bytes=67043328),
        cost_estimate=pl.CostEstimate(flops=4 * e * M * d * ff, bytes_accessed=4 * e * d * ff, transcendentals=0),
        name="layer%d" % index,
    )(tok, place, lrow, x, gate_t, dpos, rows, own3, part3, far3, w_in, w_out)


def solution(mesh):
    row_spec = P(("pod", "data", "expert"), None)
    slot_spec = P(("pod", "expert"), "data")
    weight_spec = P("expert", None, None)

    def local_fn(x, sel, gate, w_in, w_out):
        own3, part3, far3, tok, place, lrow, flag, gate_t, dpos, rows = front(sel, gate, x)
        args = (tok, place, lrow, x, gate_t, dpos, rows, own3, part3, far3, w_in, w_out)
        return lax.switch(flag[0, 0], [functools.partial(layer, k) for k in range(len(PLANS))], *args)

    return jax.shard_map(local_fn, mesh=mesh, in_specs=(row_spec, slot_spec, slot_spec, weight_spec, weight_spec), out_specs=row_spec, check_vma=False)
```

```python
import functools

import jax
import jax.numpy as jnp
from jax import lax
from jax.experimental import pallas as pl
from jax.experimental.pallas import tpu as pltpu
from jax.sharding import PartitionSpec as P

MESH = pl.DeviceIdType.MESH
VM = pl.BlockSpec(memory_space=pltpu.VMEM)
SM = pl.BlockSpec(memory_space=pltpu.SMEM)
ANY = pl.BlockSpec(memory_space=pl.ANY)
F32, BF16, I32 = jnp.float32, jnp.bfloat16, jnp.int32

LANES, SLOTS, ROWS = 128, 256, 1024
STATIC = 128
EXPERTS = 8
EARLY = 4
PLANS = ((208, 96, 128, 352, 240, 6, 4, 2, 2), (256, 256, 256, 896, 896, 1, 2, 2, 1))


def coords():
    return lax.axis_index("pod"), lax.axis_index("data"), lax.axis_index("expert")


def meet(peers):
    barrier = pltpu.get_barrier_semaphore()
    for peer in peers:
        pl.semaphore_signal(barrier, inc=1, device_id=peer, device_id_type=MESH)
    pl.semaphore_wait(barrier, len(peers))


def iota(shape, axis):
    return lax.broadcasted_iota(I32, shape, axis)


def where01(mask):
    return jnp.where(mask, 1.0, 0.0).astype(F32)


def front_kernel(sel_ref, gate_in, x_ref, own3, part3, far3, tok_ref, place_ref, lrow_ref, flag_ref, gate_ref, dpos_ref, rows_ref,
                 sel_all, gate_two, tmp32, xown, pos_scr, send, recv, gsem, csem):
    pod, i, j = coords()
    chip = j // 2
    core = lax.rem(j, 2)
    partner, across = (pod, i, j ^ 1), (pod, i, j ^ 2)
    remote = functools.partial(pltpu.make_async_remote_copy, device_id_type=MESH)
    peers = [(pod, lax.rem(i + di, 2), lax.rem(j + dj, 4)) for di in range(2) for dj in range(4) if (di, dj) != (0, 0)]
    meet(peers)
    me = i * 4 + j
    sel_all[me] = sel_ref[...]
    gate_two[i] = gate_in[...]
    shares = [remote(sel_ref, sel_all.at[me], send.at[k], recv.at[k], device_id=peer) for k, peer in enumerate(peers)]
    shares.append(remote(gate_in, gate_two.at[i], gsem.at[0], gsem.at[1], device_id=(pod, 1 - i, j)))
    for c in shares:
        c.start()

    first = remote(xown.at[pl.ds(0, STATIC)], far3.at[core], csem.at[0], csem.at[1], device_id=across)
    second = remote(far3.at[core], far3.at[core], csem.at[2], csem.at[3], device_id=partner)
    whole = remote(xown, part3, csem.at[4], csem.at[5], device_id=partner)
    keep = pltpu.make_async_copy(xown, own3, csem.at[6])

    @pl.loop(0, ROWS // LANES)
    def _(b):
        at = pl.multiple_of(b * LANES, LANES)
        for s in range(EXPERTS):
            tmp32[pl.ds(s, LANES, 8), :] = x_ref[pl.ds(at, LANES), s * LANES:(s + 1) * LANES].astype(F32)
        xown[pl.ds(at, LANES)] = tmp32[...].reshape(LANES, 8, LANES).astype(BF16)

        @pl.when(b == STATIC // LANES)
        def _():
            first.start()

    for c in shares:
        c.wait()
    whole.start()
    keep.start()

    most = jnp.zeros((8, 1), F32)
    near = jnp.zeros((8, 1), F32)
    far = jnp.zeros((8, 1), F32)
    for jj in range(4):
        s = jnp.concatenate([sel_all[jj], sel_all[4 + jj]], axis=1)
        for h in range(2):
            n = [jnp.sum(where01(s // ROWS == h * 4 + t), axis=1, keepdims=True) for t in range(4)]
            a, b = (n[:2], n[2:]) if jj < 2 else (n[2:], n[:2])
            near = jnp.maximum(near, jnp.maximum(a[0], a[1]))
            far = jnp.maximum(far, b[0] + b[1])
            most = jnp.maximum(most, a[0] + a[1] + b[0] + b[1])
    most, near, far = jnp.max(most), jnp.max(near), jnp.max(far)

    block = iota((64, LANES), 0)
    late = where01((block % 8) >= STATIC // LANES)
    upper = where01(iota((LANES, LANES), 0) < iota((LANES, LANES), 1)).astype(BF16)
    r64, c64 = iota((64, 64), 0), iota((64, 64), 1)
    lower = where01((c64 < r64) & (c64 // 8 == r64 // 8)).astype(BF16)
    gather8 = where01(iota((8, 64), 0) == iota((8, 64), 1) // 8).astype(BF16)

    def taken(his, los):
        return lax.dot_general(jnp.concatenate(his, axis=1), jnp.concatenate(los, axis=1), (((1,), (1,)), ((), ())), preferred_element_type=F32)

    def order64(mask, X):
        need = mask.astype(BF16)
        before = jnp.dot(need, upper, preferred_element_type=F32)
        offset = jnp.sum(jnp.dot(lower, need, preferred_element_type=F32), axis=1, keepdims=True)
        amount = jnp.sum(jnp.dot(gather8, need, preferred_element_type=F32), axis=1, keepdims=True)
        amount = jnp.max(jnp.where((iota((8, 1), 0) % 4) // 2 != X, amount, 0.0))
        return (before + offset).astype(I32), amount

    lists = []
    for X in range(2):
        his, los, his_e, los_e = [], [], [], []
        for d in (2 * X, 2 * X + 1, 4 + 2 * X, 5 + 2 * X):
            for e in range(EXPERTS):
                r = sel_all[d, e:e + 1, :]
                (his_e if e < EARLY else his).append(where01(block == r // LANES).astype(BF16))
                (los_e if e < EARLY else los).append(where01(iota((LANES, LANES), 0) == r % LANES).astype(BF16))
        soon = where01(taken(his_e, los_e) > 0.5) * late
        later = where01(taken(his, los) > 0.5) * late * (1.0 - soon)
        lists.append((soon, later) + order64(soon, X) + order64(later, X))
    longest_a = jnp.maximum(lists[0][3], lists[1][3])
    longest_b = jnp.maximum(lists[0][5], lists[1][5])

    plan = jnp.int32(len(PLANS) - 1)
    for p in reversed(range(len(PLANS) - 1)):
        m, co, cf, ga, gb = PLANS[p][:5]
        plan = jnp.where((most <= m) & (near <= co) & (far <= cf) & (longest_a <= ga) & (longest_b <= gb), p, plan)
    flag_ref[0, 0] = plan
    cap_a, cap_b = (jnp.int32(PLANS[-1][q]) for q in (3, 4))
    for p in range(len(PLANS) - 1):
        cap_a = jnp.where(plan == p, PLANS[p][3], cap_a)
        cap_b = jnp.where(plan == p, PLANS[p][4], cap_b)

    other = (block // 8) % 2
    row = (block % 8) * LANES + iota((64, LANES), 1)
    base = 2 * ROWS + 2 * STATIC
    places, outs = [], []
    for soon, later, pos_a, _, pos_b, _ in lists:
        listed = jnp.where(soon > 0.5, base + other * cap_a + pos_a, base + 2 * cap_a + other * cap_b + pos_b)
        places.append(jnp.where(soon + later > 0.5, listed, jnp.where(late > 0.5, 0, 2 * ROWS + other * STATIC + row)))
        outs.append(jnp.where(soon > 0.5, pos_a, jnp.where(later > 0.5, ROWS + pos_b, -1)))
    pos_scr[...] = jnp.where(chip == 0, places[0], places[1])
    far_place = pos_scr[pl.ds(pl.multiple_of(i * 32, 32), 32), :]
    block = iota((32, LANES), 0)
    tdev = block // 8
    row = (block % 8) * LANES + iota((32, LANES), 1)
    place_ref[...] = jnp.where(tdev == j, row, jnp.where(tdev == (j ^ 1), ROWS + row, far_place))

    pos_scr[...] = jnp.where(chip == 0, outs[1], outs[0])
    out_pos = pos_scr[pl.ds(pl.multiple_of((i * 4 + j) * 8, 8), 8), :]
    out_t = jnp.transpose(out_pos.astype(F32)).astype(I32)
    lane = iota((LANES, 2 * ROWS), 1)
    acc = jnp.zeros((LANES, 2 * ROWS), I32)
    for h in range(STATIC // LANES, 8):
        acc = acc + jnp.where(out_t[:, h:h + 1] == lane, iota((LANES, 1), 0) + h * LANES, 0)
    lrow_ref[...] = jnp.sum(acc, axis=0, keepdims=True)

    sel = jnp.concatenate([sel_all[j], sel_all[4 + j]], axis=1)
    gate = jnp.concatenate([gate_two[0], gate_two[1]], axis=1)
    tdev = (sel // ROWS) % 4
    row = sel % ROWS
    mine = (sel // (4 * ROWS)) == i
    upper = where01(iota((SLOTS, SLOTS), 0) < iota((SLOTS, SLOTS), 1)).astype(BF16)

    def order(mask):
        return jnp.dot(where01(mask).astype(BF16), upper, preferred_element_type=F32).astype(I32)

    rank = jnp.where(mine, order(mine), -1)
    dpos = jnp.full((EXPERTS, SLOTS), -1, I32)
    for c, mask in enumerate((tdev == j, tdev == (j ^ 1), (tdev // 2) != chip)):
        mask = mine & mask
        dpos = jnp.where(mask, order(mask) + c * SLOTS, dpos)
    packed = (sel % (4 * ROWS)) + 4 * ROWS * (dpos + 1)
    rank_t = jnp.transpose(rank.astype(F32)).astype(I32)
    packed_t = jnp.transpose(packed.astype(F32)).astype(I32)
    dpos_t = jnp.transpose(dpos.astype(F32)).astype(I32)
    row_t = jnp.transpose(((tdev % 2) * ROWS + row + 1).astype(F32)).astype(I32)
    lane = iota((SLOTS, SLOTS), 1)
    wide = iota((SLOTS, 3 * SLOTS), 1)
    toks = []
    for e in range(EXPERTS):
        toks.append(jnp.sum(jnp.where(rank_t[:, e:e + 1] == lane, packed_t[:, e:e + 1], 0), axis=0, keepdims=True))
        gate_ref[:, e:e + 1] = jnp.sum(jnp.where(rank[e:e + 1, :] == iota((SLOTS, SLOTS), 0), gate[e:e + 1, :], 0.0), axis=1, keepdims=True)
        rows_ref[e:e + 1, :] = jnp.sum(jnp.where(dpos_t[:, e:e + 1] == wide, row_t[:, e:e + 1], 0), axis=0, keepdims=True) - 1
    table = jnp.concatenate(toks, axis=0)
    tok_ref[...] = table % (4 * ROWS)
    dpos_ref[...] = table // (4 * ROWS) - 1

    first.wait_recv()
    second.start()
    first.wait_send()
    whole.wait()
    keep.wait()
    second.wait()


def front(sel, gate, x):
    e, c = sel.shape
    n, d = x.shape
    slot = jax.ShapeDtypeStruct((EXPERTS, SLOTS), I32)
    tiles = jax.ShapeDtypeStruct((n, 8, LANES), BF16)
    dma = pltpu.SemaphoreType.DMA
    return pl.pallas_call(
        front_kernel,
        out_shape=(tiles, tiles, jax.ShapeDtypeStruct((2, STATIC, 8, LANES), BF16),
                   slot, jax.ShapeDtypeStruct((32, LANES), I32), jax.ShapeDtypeStruct((1, 2 * ROWS), I32), jax.ShapeDtypeStruct((1, 1), I32),
                   jax.ShapeDtypeStruct((SLOTS, 8), F32), slot, jax.ShapeDtypeStruct((EXPERTS, 3 * SLOTS), I32)),
        in_specs=[VM, VM, VM],
        out_specs=(ANY, ANY, ANY, VM, VM, VM, SM, VM, VM, VM),
        scratch_shapes=[pltpu.VMEM((8, e, c), I32), pltpu.VMEM((2, e, c), F32), pltpu.VMEM((LANES * 8, LANES), F32), pltpu.VMEM((n, 8, LANES), BF16),
                        pltpu.VMEM((64, LANES), I32), dma((7,)), dma((7,)), dma((2,)), dma((7,))],
        compiler_params=pltpu.CompilerParams(collective_id=0, has_side_effects=True),
        name="front",
    )(sel, gate, x)


def gelu(v):
    return (0.5 * v) * (1.0 + jnp.tanh(v * (0.7978845608028654 + 0.035677408136300125 * (v * v))))


def layer_kernel(plan, tok_ref, place_ref, lrow_ref, x_ref, gate_ref, dpos_ref, rows_ref, own3, part3, far3, win_ref, wout_ref, y_ref,
                 xown, table, slist, rows32, rows16, hid0, hid1, acc, value, comb, psend, fsend, total, prow, frow, wi, wo, src, later,
                 wsem, psem, lsem, msem, csem):
    M, co, cf, cap_a, cap_b, depth, pieces_a, pieces_b, many = plan
    width = 2 * co + 2 * cf
    pod, i, j = coords()
    partner, across = (pod, i, j ^ 1), (pod, i, j ^ 2)
    core = lax.rem(j, 2)
    remote = functools.partial(pltpu.make_async_remote_copy, device_id_type=MESH)
    steps = 32

    def columns(k):
        return pl.ds(pl.multiple_of(lax.rem(k, 4) * ROWS, ROWS), ROWS)

    def first_weights(k):
        return pltpu.make_async_copy(win_ref.at[k // 4, :, columns(k)], wi.at[lax.rem(k, depth)], wsem.at[0, lax.rem(k, depth)])

    def second_weights(k):
        return pltpu.make_async_copy(wout_ref.at[k // 4, columns(k), :], wo.at[lax.rem(k, depth)], wsem.at[1, lax.rem(k, depth)])

    load = pltpu.make_async_copy(own3, xown, psem.at[0])
    base = 2 * ROWS + 2 * STATIC
    loads = [pltpu.make_async_copy(own3, table.at[pl.ds(0, ROWS)], psem.at[1]),
             pltpu.make_async_copy(part3, table.at[pl.ds(ROWS, ROWS)], psem.at[2]),
             pltpu.make_async_copy(far3.at[0], table.at[pl.ds(2 * ROWS, STATIC)], psem.at[3]),
             pltpu.make_async_copy(far3.at[1], table.at[pl.ds(2 * ROWS + STATIC, STATIC)], psem.at[4])]
    load.start()
    for c in loads:
        c.start()

    @pl.loop(0, depth)
    def _(k):
        first_weights(k).start()
        second_weights(k).start()

    meet([partner, across])
    small = [remote(rows_ref, prow, psem.at[5], psem.at[6], device_id=partner),
             remote(rows_ref, frow.at[core], psem.at[7], psem.at[8], device_id=across)]
    for c in small:
        c.start()

    def list_copies(start, size, pieces, sem, into):
        n = size // pieces
        out = []
        for k in range(pieces):
            there = into(pl.ds(k * n, n), k * n, n)
            out.append((remote(slist.at[pl.ds(start + k * n, n)], there, sem.at[0, k], sem.at[1, k], device_id=across),
                        remote(there, there, sem.at[2, k], sem.at[3, k], device_id=partner)))
        return out

    mine = base + core * cap_a
    lists_a = list_copies(0, cap_a, pieces_a, lsem, lambda rows, at, n: table.at[pl.ds(mine + at, n)])
    lists_b = list_copies(cap_a, cap_b, pieces_b, msem, lambda rows, at, n: later.at[core, rows])
    load.wait()
    held = None
    for start, size, pieces, copies, index in ((0, cap_a, pieces_a, lists_a, 0), (cap_a, cap_b, pieces_b, lists_b, ROWS)):
        n = size // pieces
        for k in range(pieces):
            @pl.loop(0, n // 8)
            def _(b):
                at = k * n + b * 8
                tiles = [xown[lrow_ref[0, index + at + u]] for u in range(EXPERTS)]
                for u, tile in enumerate(tiles):
                    slist[start + at + u] = tile

            if held is not None:
                held.start()
            held = copies[k][0]
    total[...] = x_ref[...].astype(F32)
    held.start()

    @pl.loop(0, 8)
    def _(e):
        @pl.loop(0, M // 16)
        def _(b):
            for u in range(16):
                tok = tok_ref[e, b * 16 + u]
                src[e, b * 16 + u] = place_ref[tok >> 7, tok & (LANES - 1)]

    small[1].wait()
    pass_rows = remote(frow.at[core], frow.at[core], psem.at[9], psem.at[10], device_id=partner)
    pass_rows.start()
    for send, forward in lists_a:
        send.wait_recv()
        forward.start()
    small[0].wait()
    pass_rows.wait()
    for c in loads:
        c.wait()
    for send, forward in lists_a:
        send.wait_send()
        forward.wait()

    def fetch(e, slot, f):
        at = pl.multiple_of(jnp.minimum(f * 64, M - 64), 16)
        for v in range(0, 64, 16):
            tiles = [table[src[e, at + v + u]].astype(F32) for u in range(16)]
            for u, tile in enumerate(tiles):
                rows32[(v + u) * 8:(v + u + 1) * 8, :] = tile
        for s in range(EXPERTS):
            rows16[slot, pl.ds(at, 64), s * LANES:(s + 1) * LANES] = rows32[pl.ds(s, 64, 8), :].astype(BF16)

    @pl.loop(0, 4)
    def _(f):
        fetch(0, 0, f)

    def near(e):
        slot = lax.rem(e, 4)
        return remote(psend.at[slot], comb.at[pl.ds(e * width + co, co)], csem.at[0, e], csem.at[1, e], device_id=partner)

    def far(e):
        slot = lax.rem(e, 4)
        return remote(fsend.at[slot], comb.at[pl.ds(e * width + 2 * co + core * cf, cf)], csem.at[2, e], csem.at[3, e], device_id=across)

    def passed(e):
        there = comb.at[pl.ds(e * width + 2 * co + core * cf, cf)]
        return remote(there, there, csem.at[4, e], csem.at[5, e], device_id=partner)

    def finish(e):
        cols = gate_ref[...]
        weight = jnp.sum(jnp.where(iota(cols.shape, 1) == e, cols, 0.0), axis=1, keepdims=True)[:M]
        value[...] = (weight * acc[...]).astype(BF16)
        d = dpos_ref[pl.ds(e, 1), :][:, :M]
        kind, rank = d >> 8, d & (SLOTS - 1)
        d = jnp.where(d < 0, -1, rank + jnp.where(kind == 0, 0, jnp.where(kind == 1, co, 2 * co)))
        sort = where01(iota((2 * co + cf, M), 0) == d).astype(BF16)
        slot = lax.rem(e, 4)
        lists = jnp.dot(sort, value[...], preferred_element_type=F32).astype(BF16)
        comb[pl.ds(pl.multiple_of(e * width, 16), co), :] = lists[:co]
        psend[slot] = lists[co:2 * co]
        fsend[slot] = lists[2 * co:]

    def take(e):
        far(e).wait_recv()
        passed(e).start()

    def add(e):
        rows = []
        for m in range(e, e + many):
            passed(m).wait_recv()
            near(m).wait_recv()
            rows += [rows_ref[m:m + 1, :co], prow[m:m + 1, SLOTS:SLOTS + co],
                     frow[0, m:m + 1, 2 * SLOTS:2 * SLOTS + cf], frow[1, m:m + 1, 2 * SLOTS:2 * SLOTS + cf]]
        rows = jnp.concatenate(rows, axis=1) - core * ROWS

        @pl.loop(0, 2)
        def _(b):
            at = pl.multiple_of(b * 2 * SLOTS, 2 * SLOTS)
            put = where01(iota((2 * SLOTS, many * width), 0) + at == rows).astype(BF16)
            total[pl.ds(at, 2 * SLOTS), :] += jnp.dot(put, comb[e * width:(e + many) * width, :], preferred_element_type=F32)

    def first(k, hid):
        xs = rows16[lax.rem(k // 4, 2)]
        for s in range(4):
            u = jnp.dot(xs, wi[lax.rem(k, depth), :, s * SLOTS:(s + 1) * SLOTS], preferred_element_type=F32)
            hid[:, s * SLOTS:(s + 1) * SLOTS] = gelu(u).astype(BF16)

    def second(k, hid):
        out = jnp.dot(hid[...], wo[lax.rem(k, depth)], preferred_element_type=F32)
        acc[...] = jnp.where(lax.rem(k, 4) == 0, out, acc[...] + out)

    def step(k, new, old):
        e = k // 4
        first_weights(k).wait()

        @pl.when(k != 1)
        def _():
            second_weights(jnp.maximum(k - 1, 0)).wait()

        first(k, new)
        second(jnp.maximum(k - 1, 0), old)
        fetch(jnp.minimum(e + 1, 7), 1 - lax.rem(e, 2), lax.rem(k, 4))

        @pl.when(k + depth < steps)
        def _():
            first_weights(k + depth).start()

        @pl.when((k > 0) & (k - 1 + depth < steps))
        def _():
            second_weights(k - 1 + depth).start()

    @pl.loop(0, steps // 2)
    def _(kk):
        k = 2 * kk
        e = kk // 2
        even = lax.rem(kk, 2) == 0
        for q, (send, forward) in enumerate(lists_b):
            @pl.when(kk == 2 * EARLY - 2 - len(lists_b) + q)
            def _():
                send.wait_recv()
                forward.start()

        @pl.when(kk == 2 * EARLY - 2)
        def _():
            for send, forward in lists_b:
                send.wait_send()
                forward.wait()
            for side in range(2):
                @pl.loop(0, cap_b // 16)
                def _(b):
                    table[pl.ds(base + 2 * cap_a + side * cap_b + b * 16, 16)] = later[side, pl.ds(b * 16, 16)]

        step(k, hid0, hid1)

        @pl.when(even & (e >= 1))
        def _():
            @pl.when(e >= 5)
            def _():
                near(e - 5).wait_send()
                far(e - 5).wait_send()

            finish(e - 1)

        @pl.when((~even) & (e >= 4))
        def _():
            take(e - 4)

        step(k + 1, hid1, hid0)

        @pl.when(even & (e >= 1))
        def _():
            far(e - 1).start()
            near(e - 1).start()

    second_weights(steps - 1).wait()
    second(steps - 1, hid1)
    near(3).wait_send()
    far(3).wait_send()
    finish(7)
    take(4)
    far(7).start()
    near(7).start()
    take(5)
    add(0)
    if many == 1:
        add(1)
    take(6)
    for m in range(2, EXPERTS - many, many):
        add(m)
    take(7)
    add(EXPERTS - many)
    for e in range(EXPERTS):
        if e >= 4:
            near(e).wait_send()
            far(e).wait_send()
        passed(e).wait_send()
    y_ref[...] = total[...].astype(BF16)


def layer(index, tok, place, lrow, x, gate_t, dpos, rows, own3, part3, far3, w_in, w_out):
    plan = PLANS[index]
    M, co, cf, cap_a, cap_b, depth, pieces_a, pieces_b, many = plan
    n, d = x.shape
    e, _, ff = w_in.shape
    dma = pltpu.SemaphoreType.DMA
    vm = pltpu.VMEM
    return pl.pallas_call(
        functools.partial(layer_kernel, plan),
        out_shape=jax.ShapeDtypeStruct((n, d), BF16),
        in_specs=[SM, SM, SM, VM, VM, VM, VM, ANY, ANY, ANY, ANY, ANY],
        out_specs=VM,
        scratch_shapes=[vm((n, 8, LANES), BF16), vm((2 * (ROWS + STATIC + cap_a + cap_b), 8, LANES), BF16), vm((cap_a + cap_b, 8, LANES), BF16),
                        vm((64 * 8, LANES), F32), vm((2, M, d), BF16), vm((M, ROWS), BF16), vm((M, ROWS), BF16), vm((M, d), F32), vm((M, d), BF16),
                        vm((8 * (2 * co + 2 * cf), d), BF16), vm((4, co, d), BF16), vm((4, cf, d), BF16), vm((n, d), F32),
                        vm((EXPERTS, 3 * SLOTS), I32), vm((2, 8, 3 * SLOTS), I32), vm((depth, d, ROWS), BF16), vm((depth, ROWS, d), BF16),
                        pltpu.SMEM((EXPERTS, SLOTS), I32), vm((2, cap_b, 8, LANES), BF16),
                        dma((2, depth)), dma((11,)), dma((4, pieces_a)), dma((4, pieces_b)), dma((6, 8))],
        compiler_params=pltpu.CompilerParams(collective_id=1 + index, has_side_effects=True, vmem_limit_bytes=67043328),
        cost_estimate=pl.CostEstimate(flops=4 * e * M * d * ff, bytes_accessed=4 * e * d * ff, transcendentals=0),
        name="layer%d" % index,
    )(tok, place, lrow, x, gate_t, dpos, rows, own3, part3, far3, w_in, w_out)


def solution(mesh):
    row_spec = P(("pod", "data", "expert"), None)
    slot_spec = P(("pod", "expert"), "data")
    weight_spec = P("expert", None, None)

    def local_fn(x, sel, gate, w_in, w_out):
        own3, part3, far3, tok, place, lrow, flag, gate_t, dpos, rows = front(sel, gate, x)
        args = (tok, place, lrow, x, gate_t, dpos, rows, own3, part3, far3, w_in, w_out)
        return lax.switch(flag[0, 0], [functools.partial(layer, k) for k in range(len(PLANS))], *args)

    return jax.shard_map(local_fn, mesh=mesh, in_specs=(row_spec, slot_spec, slot_spec, weight_spec, weight_spec), out_specs=row_spec, check_vma=False)
```
